32 devices in a mesh: seq: 16 (over z, x, core), head: 2 (over y).
Axes of the slice: x: 2, y: 2, z: 4, core: 2. Of those that a mesh axis runs over, the one named last changes fastest.
Arguments:
- tokens: bfloat16 [8192, 4096], P('seq', 'head'), may hold values from -64 to 64
- norm_gain: float32 [4096], replicated, may hold values from 0.5 to 1.5
- w_query: bfloat16 [4096, 4096], P(None, 'head'), may hold values from -4 to 4
- w_key: bfloat16 [4096, 1024], P(None, 'head'), may hold values from -4 to 4
- w_value: bfloat16 [4096, 1024], P(None, 'head'), may hold values from -0.09375 to 0.09375
- w_output: bfloat16 [4096, 4096], P('head'), may hold values from -0.09375 to 0.09375
- widths: int32 [64], P('seq'), may hold values from 1 to 32
- dilation: int32 [64, 8], replicated, may hold values from 0 to 63, as said below
Outputs:
- layer_out: bfloat16 [8192, 4096], P('seq', 'head')
The draws below stay inside these ranges and needn't reach their ends.
Inputs may be any that keep to these rules, and one draw needn't show every extreme that they name: `dilation`: the 8 entries of one row differ. Over the 4 aligned rows of one index of seq, all entries that fall into the blocks of one index of seq (ids k * 4 to k * 4 + 3) name the same block. Row i names blocks of the indices 0 to max(i // 4, 8) - 1 of seq only.
All inputs are finite; a program needn't handle non-finite values.
Results may differ from the reference program's by a relative error of at most 0.005.
Values may be sent and summed in bfloat16 or wider, within the bound.
A program may use at most 128 MiB of HBM per device.

```python
import math
import jax
import jax.numpy as jnp
from jax import lax

MODEL_WIDTH = 4096
QUERY_HEADS = 32
KEY_VALUE_HEADS = 8
HEAD_WIDTH = 128
BLOCK_TOKENS = 128
WINDOW_BLOCKS = 32
DILATION_COUNT = 8
QB_DEV = 4
NBLK = 64
TOKENS = 8192
QCOLS = 4096
KVCOLS = 1024


def draw_tokens(key, part):
    values = jax.random.normal(jax.random.fold_in(key, 4), (TOKENS, MODEL_WIDTH), jnp.float32)
    return jnp.clip(values, -64.0, 64.0).astype(jnp.bfloat16)


def key_projection_matrix(key):
    return jax.random.normal(jax.random.fold_in(key, 21), (MODEL_WIDTH, KEY_VALUE_HEADS * HEAD_WIDTH), jnp.float32) / math.sqrt(MODEL_WIDTH)


def draw_w_key(key, part):
    return jnp.clip(key_projection_matrix(key), -4.0, 4.0).astype(jnp.bfloat16)


def draw_w_query(key, part):
    noise_part = jax.random.normal(jax.random.fold_in(key, 22), (MODEL_WIDTH, QUERY_HEADS * HEAD_WIDTH), jnp.float32) / math.sqrt(MODEL_WIDTH)
    values = noise_part
    return jnp.clip(values, -4.0, 4.0).astype(jnp.bfloat16)


def draw_dilation(key, part):
    devices = NBLK // QB_DEV
    local_picks = jax.random.randint(jax.random.fold_in(key, 11), (devices, devices), 0, QB_DEV)
    scores = jax.random.randint(jax.random.fold_in(key, 12), (NBLK, devices), 0, 1 << 20)
    block_ids = jnp.arange(NBLK, dtype=jnp.int32)
    requester = block_ids // QB_DEV
    owner_limit = jnp.maximum(requester, DILATION_COUNT)
    owners = jnp.arange(devices, dtype=jnp.int32)
    ranked = scores * devices + owners[None, :] + jnp.where(owners[None, :] >= owner_limit[:, None], (1 << 20) * devices, 0)
    ordered = jnp.argsort(ranked, axis=1)[:, :DILATION_COUNT].astype(jnp.int32)
    chosen = local_picks[requester[:, None], ordered]
    return (ordered * QB_DEV + chosen).astype(jnp.int32)


def with_ends(drawn, own_key, low, high):
    dims = drawn.shape
    index_at = [jax.random.randint(jax.random.fold_in(own_key, axis), (), 0, dims[axis]) for axis in range(len(dims))]
    drawn = drawn.at[tuple(index_at)].set(low)
    longest = dims.index(max(dims))
    index_at[longest] = (index_at[longest] + 1) % dims[longest]
    return drawn.at[tuple(index_at)].set(high)


def block_scale(own_key, shape, pieces, low, top_value):
    def one(axis_at, blocks):
        steps = jax.random.uniform(jax.random.fold_in(jax.random.fold_in(own_key, 6), axis_at), (blocks,), jnp.float32, low / len(pieces), top_value / len(pieces))
        return jnp.repeat(jnp.exp(steps), shape[axis_at] // blocks).reshape((-1,) + (1,) * (len(shape) - axis_at - 1))

    level = one(*pieces[0])
    for cut in pieces[1:]:
        level = level * one(*cut)
    return level


def gaussian(key, shape, width, limit, shards=(), kind=jnp.bfloat16):
    drawn = jax.random.normal(key, shape, jnp.float32) * width
    if len(shards) > 0:
        drawn = block_scale(key, shape, shards, -0.22, 0.18) * drawn
    return jnp.clip(drawn, min=-limit, max=limit).astype(kind)


def setup_inputs(seed: int = 0) -> dict:
    arg_keys = jax.random.split(jax.random.key(seed), 9)
    tokens = draw_tokens(jax.random.fold_in(arg_keys[8], 71), 0)
    norm_gain = jnp.clip(1.0 + 0.1 * jax.random.normal(arg_keys[1], (MODEL_WIDTH,), jnp.float32), 0.5, 1.5)
    w_query = draw_w_query(jax.random.fold_in(arg_keys[8], 71), 0)
    w_key = draw_w_key(jax.random.fold_in(arg_keys[8], 71), 0)
    w_value = gaussian(arg_keys[4], (MODEL_WIDTH, KVCOLS), MODEL_WIDTH ** -0.5, 0.09375, ((1, 2),))
    w_output = gaussian(arg_keys[5], (QCOLS, MODEL_WIDTH), QCOLS ** -0.5, 0.09375, ((0, 2),))
    widths = with_ends(jax.random.randint(arg_keys[6], (NBLK,), 1, WINDOW_BLOCKS + 1), jax.random.fold_in(arg_keys[6], 1), 1, WINDOW_BLOCKS).astype(jnp.int32)
    dilation = draw_dilation(jax.random.fold_in(arg_keys[8], 71), 0)
    return {"tokens": tokens, "norm_gain": norm_gain, "w_query": w_query, "w_key": w_key, "w_value": w_value, "w_output": w_output, "widths": widths, "dilation": dilation}


EPSILON = 1e-05
NEGATIVE = -1e+30
ROPE_BASE = 10000.0

def rotary(values, positions, head_size):
    row_count = values.shape[0]
    head_count = values.shape[1] // head_size
    half_size = head_size // 2
    frequency = ROPE_BASE ** (-jnp.arange(half_size, dtype=jnp.float32) * 2.0 / head_size)
    angles = positions.astype(jnp.float32)[:, None] * frequency[None, :]
    cosine = jnp.cos(angles)[:, None, :]
    sine_part = jnp.sin(angles)[:, None, :]
    shaped = values.reshape(row_count, head_count, head_size)
    first_half = shaped[:, :, :half_size]
    second = shaped[:, :, half_size:]
    rotated = jnp.concatenate([first_half * cosine - second * sine_part, second * cosine + first_half * sine_part], axis=2)
    return rotated.reshape(row_count, head_count * head_size)

def rms_rows(tokens, norm_gain):
    values = tokens.astype(jnp.float32)
    scale_row = lax.rsqrt(lax.optimization_barrier(jnp.mean(values * values, axis=1, keepdims=True)) + EPSILON)
    return (values * scale_row * norm_gain[None, :]).astype(jnp.bfloat16)

def reference(tokens, norm_gain, w_query, w_key, w_value, w_output, widths, dilation):
    total_rows = tokens.shape[0]
    count_of_blocks = total_rows // BLOCK_TOKENS
    query_group_width = QUERY_HEADS // KEY_VALUE_HEADS
    normed = rms_rows(tokens, norm_gain)
    positions = jnp.arange(total_rows, dtype=jnp.int32)
    query_rows = rotary(jnp.dot(normed, w_query, preferred_element_type=jnp.float32), positions, HEAD_WIDTH).astype(jnp.bfloat16)
    key_row_list = rotary(jnp.dot(normed, w_key, preferred_element_type=jnp.float32), positions, HEAD_WIDTH).astype(jnp.bfloat16)
    value_row_list = jnp.dot(normed, w_value, preferred_element_type=jnp.float32).astype(jnp.bfloat16)
    leading_zero_rows = jnp.zeros(((WINDOW_BLOCKS - 1) * BLOCK_TOKENS, KEY_VALUE_HEADS * HEAD_WIDTH), jnp.bfloat16)
    key_padded = jnp.concatenate([leading_zero_rows, key_row_list], axis=0)
    value_padded = jnp.concatenate([leading_zero_rows, value_row_list], axis=0)
    blocked_keys = key_row_list.reshape(count_of_blocks, BLOCK_TOKENS, KEY_VALUE_HEADS * HEAD_WIDTH)
    blocked_values = value_row_list.reshape(count_of_blocks, BLOCK_TOKENS, KEY_VALUE_HEADS * HEAD_WIDTH)
    offsets = jnp.arange(BLOCK_TOKENS, dtype=jnp.int32)
    near_ids = jnp.arange(WINDOW_BLOCKS, dtype=jnp.int32) - (WINDOW_BLOCKS - 1)
    score_scale = 1.0 / math.sqrt(HEAD_WIDTH)

    def one_block(block_index):
        window_low = block_index - widths[block_index] + 1
        current_query_block = lax.dynamic_slice_in_dim(query_rows, block_index * BLOCK_TOKENS, BLOCK_TOKENS, 0)
        near_keys = lax.dynamic_slice_in_dim(key_padded, block_index * BLOCK_TOKENS, WINDOW_BLOCKS * BLOCK_TOKENS, 0)
        near_values = lax.dynamic_slice_in_dim(value_padded, block_index * BLOCK_TOKENS, WINDOW_BLOCKS * BLOCK_TOKENS, 0)
        distant_block_ids = dilation[block_index]
        distant_keys = jnp.take(blocked_keys, distant_block_ids, axis=0).reshape(DILATION_COUNT * BLOCK_TOKENS, KEY_VALUE_HEADS * HEAD_WIDTH)
        distant_values = jnp.take(blocked_values, distant_block_ids, axis=0).reshape(DILATION_COUNT * BLOCK_TOKENS, KEY_VALUE_HEADS * HEAD_WIDTH)
        key_slice = jnp.concatenate([near_keys, distant_keys], axis=0)
        value_slice = jnp.concatenate([near_values, distant_values], axis=0)
        block_ids = jnp.concatenate([block_index + near_ids, distant_block_ids])
        block_ok = jnp.concatenate([block_index + near_ids >= jnp.maximum(window_low, 0), distant_block_ids < window_low])
        key_pos = jnp.repeat(block_ids, BLOCK_TOKENS) * BLOCK_TOKENS + jnp.tile(offsets, WINDOW_BLOCKS + DILATION_COUNT)
        query_pos = block_index * BLOCK_TOKENS + offsets
        allowed = jnp.repeat(block_ok, BLOCK_TOKENS)[None, :] & (key_pos[None, :] <= query_pos[:, None])
        query_single_float = current_query_block.astype(jnp.float32).reshape(BLOCK_TOKENS, KEY_VALUE_HEADS, query_group_width, HEAD_WIDTH)
        key_single_float = key_slice.astype(jnp.float32).reshape(-1, KEY_VALUE_HEADS, HEAD_WIDTH)
        value_single_float = value_slice.astype(jnp.float32).reshape(-1, KEY_VALUE_HEADS, HEAD_WIDTH)
        scores = jnp.einsum('qhgd,khd->hgqk', query_single_float, key_single_float) * score_scale
        scores = jnp.where(allowed[None, None, :, :], scores, NEGATIVE)
        top_now = lax.optimization_barrier(jnp.max(scores, axis=3, keepdims=True))
        weights = jnp.exp(scores - top_now)
        total_sum = lax.optimization_barrier(jnp.sum(weights, axis=3))
        prob_bf = lax.optimization_barrier(weights.astype(jnp.bfloat16)).astype(jnp.float32)
        mixed = jnp.einsum('hgqk,khd->qhgd', prob_bf, value_single_float)
        mixed = mixed / jnp.transpose(total_sum, (2, 0, 1))[:, :, :, None]
        return mixed.reshape(BLOCK_TOKENS, QUERY_HEADS * HEAD_WIDTH)
    attention = lax.map(one_block, jnp.arange(count_of_blocks, dtype=jnp.int32))
    attention = attention.reshape(total_rows, QUERY_HEADS * HEAD_WIDTH).astype(jnp.bfloat16)
    projected = jnp.dot(attention, w_output, preferred_element_type=jnp.float32)
    return (tokens.astype(jnp.float32) + projected).astype(jnp.bfloat16)
```

```python
import functools
import math

import jax
import jax.numpy as jnp
from jax import lax
from jax.experimental import pallas as pl
from jax.experimental.pallas import tpu as pltpu
from jax.sharding import PartitionSpec as P

MODEL_WIDTH = 4096
HEAD_WIDTH = 128
BLOCK_TOKENS = 128
WINDOW_BLOCKS = 32
TURN = 4
PAIR = 2

EPSILON = 1e-05
NEGATIVE = -1e30
ROPE_BASE = 10000.0
SCORE_SCALE = math.log2(math.e) / math.sqrt(HEAD_WIDTH)
VMEM_BYTES = 48 * 1024 * 1024
EXCHANGE_VMEM = 60 * 1024 * 1024
PLANE = 4
QUERY_TILE = 256
MESH = pl.DeviceIdType.MESH


def turned(values, cosine, sine_part):
    return values * cosine + pltpu.roll(values, HEAD_WIDTH // 2, 1) * sine_part


def rope_kernel(heads, part_heads, chunks, *refs):
    key_refs, value_refs = refs[:chunks], refs[chunks : 2 * chunks]
    cos_ref, sin_ref = refs[2 * chunks : 2 * chunks + 2]
    outs = refs[2 * chunks + 2 :]
    for chunk in range(chunks):
        rows = key_refs[chunk].shape[0]
        span = pl.ds(chunk * rows, rows)
        cosine, sine_part = cos_ref[span, :], sin_ref[span, :]
        for head in range(heads):
            part, slot = divmod(head, part_heads)
            columns = slice(head * HEAD_WIDTH, (head + 1) * HEAD_WIDTH)
            outs[part][slot, span, :] = turned(key_refs[chunk][:, columns], cosine, sine_part).astype(
                jnp.bfloat16
            )
            outs[part][part_heads + slot, span, :] = value_refs[chunk][:, columns].astype(jnp.bfloat16)


def attention_kernel(
    first, groups, ids_ref, count_ref, q_ref, cos_ref, sin_ref, k_ref, v_ref, o_ref, q_s, m_s, l_s, acc_s
):
    block = pl.program_id(1) + first
    listed = count_ref[block]
    last = ids_ref.shape[1] - 1
    pair = PAIR if groups % PAIR == 0 else 1
    height = pair * BLOCK_TOKENS
    cosine, sine_part = cos_ref[...], sin_ref[...]
    for group in range(groups):
        u = q_ref[:, group * HEAD_WIDTH : (group + 1) * HEAD_WIDTH]
        q_s[pl.ds(group * BLOCK_TOKENS, BLOCK_TOKENS), :] = turned(u, cosine, sine_part).astype(
            jnp.bfloat16
        )

    def rows_of(ref, index):
        return ref[0, pl.ds(pl.multiple_of(index * BLOCK_TOKENS, BLOCK_TOKENS), BLOCK_TOKENS), :]

    def lane_sum(weights):
        total = weights[:, :HEAD_WIDTH]
        for at in range(1, weights.shape[1] // HEAD_WIDTH):
            total = total + weights[:, at * HEAD_WIDTH : (at + 1) * HEAD_WIDTH]
        return total

    own = ids_ref[block, last]
    key_own, value_own = rows_of(k_ref, own), rows_of(v_ref, own)
    row_at = lax.broadcasted_iota(jnp.int32, (height, BLOCK_TOKENS), 0) % BLOCK_TOKENS
    col_at = lax.broadcasted_iota(jnp.int32, (height, BLOCK_TOKENS), 1)
    causal = col_at <= row_at
    for at in range(groups // pair):
        span = pl.ds(at * height, height)
        scores = lax.dot_general(
            q_s[span, :], key_own, (((1,), (1,)), ((), ())), preferred_element_type=jnp.float32
        )
        scores = jnp.where(causal, scores, NEGATIVE)
        top = jnp.max(scores, axis=1, keepdims=True)
        weights = jnp.exp2((scores - top) * SCORE_SCALE)
        m_s[span, :] = jnp.broadcast_to(top, (height, HEAD_WIDTH))
        l_s[span, :] = weights
        acc_s[span, :] = jnp.dot(
            weights.astype(jnp.bfloat16), value_own, preferred_element_type=jnp.float32
        )

    def turn(index, masked):
        base = index * TURN
        ids = [ids_ref[block, base + at] for at in range(TURN)]
        keys = jnp.concatenate([rows_of(k_ref, one) for one in ids], axis=0)
        values = jnp.concatenate([rows_of(v_ref, one) for one in ids], axis=0)
        for at in range(groups // pair):
            span = pl.ds(at * height, height)
            scores = lax.dot_general(
                q_s[span, :], keys, (((1,), (1,)), ((), ())), preferred_element_type=jnp.float32
            )
            if masked:
                column = lax.broadcasted_iota(jnp.int32, scores.shape, 1)
                scores = jnp.where(column < (listed - base) * BLOCK_TOKENS, scores, NEGATIVE)
            top_prev = m_s[span, :]
            top = jnp.maximum(top_prev, jnp.max(scores, axis=1, keepdims=True))
            factor = jnp.exp2((top_prev - top) * SCORE_SCALE)
            weights = jnp.exp2((scores - jnp.concatenate([top] * TURN, axis=1)) * SCORE_SCALE)
            m_s[span, :] = top
            l_s[span, :] = l_s[span, :] * factor + lane_sum(weights)
            acc_s[span, :] = acc_s[span, :] * factor + jnp.dot(
                weights.astype(jnp.bfloat16), values, preferred_element_type=jnp.float32
            )

    whole_turns = listed // TURN

    @pl.loop(0, whole_turns)
    def _(index):
        turn(index, False)

    @pl.when(listed > whole_turns * TURN)
    def _():
        turn(whole_turns, True)

    for group in range(groups):
        span = pl.ds(group * BLOCK_TOKENS, BLOCK_TOKENS)
        total = jnp.sum(l_s[span, :], axis=1, keepdims=True)
        o_ref[:, group * HEAD_WIDTH : (group + 1) * HEAD_WIDTH] = (acc_s[span, :] / total).astype(
            jnp.bfloat16
        )


def attention_call(query_raw, cosine, sine_part, gathered, ids, counts, first, part, part_heads, groups):
    blocks = query_raw.shape[0] // BLOCK_TOKENS
    tokens_all = gathered.shape[1]
    width = groups * HEAD_WIDTH
    grid_spec = pltpu.PrefetchScalarGridSpec(
        num_scalar_prefetch=2,
        grid=(part_heads, blocks),
        in_specs=[
            pl.BlockSpec((BLOCK_TOKENS, width), lambda h, b, *_: (b, part * part_heads + h)),
            pl.BlockSpec((BLOCK_TOKENS, HEAD_WIDTH), lambda h, b, *_: (first + b, 0)),
            pl.BlockSpec((BLOCK_TOKENS, HEAD_WIDTH), lambda h, b, *_: (first + b, 0)),
            pl.BlockSpec((1, tokens_all, HEAD_WIDTH), lambda h, b, *_: (h, 0, 0)),
            pl.BlockSpec((1, tokens_all, HEAD_WIDTH), lambda h, b, *_: (part_heads + h, 0, 0)),
        ],
        out_specs=pl.BlockSpec((BLOCK_TOKENS, width), lambda h, b, *_: (b, h)),
        scratch_shapes=[
            pltpu.VMEM((groups * BLOCK_TOKENS, HEAD_WIDTH), jnp.bfloat16),
            pltpu.VMEM((groups * BLOCK_TOKENS, HEAD_WIDTH), jnp.float32),
            pltpu.VMEM((groups * BLOCK_TOKENS, HEAD_WIDTH), jnp.float32),
            pltpu.VMEM((groups * BLOCK_TOKENS, HEAD_WIDTH), jnp.float32),
        ],
    )
    pairs = part_heads * groups * blocks * BLOCK_TOKENS * BLOCK_TOKENS * WINDOW_BLOCKS
    return pl.pallas_call(
        functools.partial(attention_kernel, first, groups),
        grid_spec=grid_spec,
        out_shape=jax.ShapeDtypeStruct((blocks * BLOCK_TOKENS, part_heads * width), jnp.bfloat16),
        compiler_params=pltpu.CompilerParams(
            dimension_semantics=("arbitrary", "arbitrary"), vmem_limit_bytes=VMEM_BYTES
        ),
        cost_estimate=pl.CostEstimate(
            flops=pairs * HEAD_WIDTH * 4, bytes_accessed=gathered.size * 2, transcendentals=pairs
        ),
        name="attention",
    )(ids, counts, query_raw, cosine, sine_part, gathered, gathered)


def block_lists(first_block, count_of_blocks, widths, dilation):
    block = first_block + jnp.arange(count_of_blocks, dtype=jnp.int32)
    window_low = block - widths + 1
    start = jnp.maximum(window_low, 0)
    near = block - start
    far = lax.dynamic_slice_in_dim(dilation, first_block, count_of_blocks, 0)
    valid = far < window_low[:, None]
    far_count = far.shape[1]
    earlier = jnp.tril(jnp.ones((far_count, far_count), jnp.int32), -1)
    rank = near[:, None] + jnp.sum(valid.astype(jnp.int32)[:, None, :] * earlier[None], axis=2)
    length = -(-(WINDOW_BLOCKS + far_count) // TURN) * TURN
    place = jnp.arange(length, dtype=jnp.int32)
    hit = valid[:, :, None] & (rank[:, :, None] == place[None, None, :])
    ids = jnp.sum(jnp.where(hit, far[:, :, None], 0), axis=1)
    ids = ids + jnp.where(place[None, :] < near[:, None], start[:, None] + place[None, :], 0)
    ids = jnp.concatenate([ids, block[:, None]], axis=1)
    counts = near + jnp.sum(valid.astype(jnp.int32), axis=1)
    return ids, counts


def general_shards(tokens, norm_gain, w_query, w_key, w_value, w_output, widths, dilation):
    row_count, width_own = tokens.shape
    count_of_blocks = row_count // BLOCK_TOKENS
    seq_index = lax.axis_index("seq")
    head_index = lax.axis_index("head")
    head_count = lax.axis_size("head")
    first_block = seq_index * count_of_blocks
    swap = [(0, 1), (1, 0)]
    chunks = 2 if count_of_blocks % 2 == 0 else 1
    rows = row_count // chunks
    kv_heads = w_key.shape[1] // HEAD_WIDTH
    groups = w_query.shape[1] // w_key.shape[1]
    parts = 2 if kv_heads % 2 == 0 else 1
    part_heads = kv_heads // parts

    own_tokens = [tokens[chunk * rows : (chunk + 1) * rows] for chunk in range(chunks)]
    if head_count == 2:
        sent = [lax.ppermute(one, "head", swap) for one in own_tokens]
        flip = head_index == 1
        full_tokens = [
            jnp.concatenate([jnp.where(flip, other, own), jnp.where(flip, own, other)], axis=1)
            for own, other in zip(own_tokens, sent)
        ]
    else:
        full = lax.all_gather(tokens, "head", axis=1, tiled=True)
        full_tokens = [full[chunk * rows : (chunk + 1) * rows] for chunk in range(chunks)]

    half = HEAD_WIDTH // 2
    lane = jnp.arange(HEAD_WIDTH, dtype=jnp.int32)
    frequency = ROPE_BASE ** (-(lane % half).astype(jnp.float32) * 2.0 / HEAD_WIDTH)
    positions = first_block * BLOCK_TOKENS + jnp.arange(row_count, dtype=jnp.int32)
    angles = positions.astype(jnp.float32)[:, None] * frequency[None, :]
    cosine = jnp.cos(angles)
    sine_part = jnp.sin(angles) * jnp.where(lane < half, -1.0, 1.0)[None, :]
    ids, counts = block_lists(first_block, count_of_blocks, widths, dilation)

    queries, keys, values = [], [], []
    for one in full_tokens:
        wide = one.astype(jnp.float32)
        mean = jnp.sum(wide * wide, axis=1, keepdims=True) / MODEL_WIDTH
        normed = (wide * lax.rsqrt(mean + EPSILON) * norm_gain[None, :]).astype(jnp.bfloat16)
        keys.append(jnp.dot(normed, w_key, preferred_element_type=jnp.float32))
        values.append(jnp.dot(normed, w_value, preferred_element_type=jnp.float32))
        queries.append(jnp.dot(normed, w_query, preferred_element_type=jnp.float32))

    pairs = pl.pallas_call(
        functools.partial(rope_kernel, kv_heads, part_heads, chunks),
        out_shape=[jax.ShapeDtypeStruct((2 * part_heads, row_count, HEAD_WIDTH), jnp.bfloat16)] * parts,
        compiler_params=pltpu.CompilerParams(vmem_limit_bytes=VMEM_BYTES),
        cost_estimate=pl.CostEstimate(
            flops=8 * row_count * kv_heads * HEAD_WIDTH,
            bytes_accessed=12 * row_count * kv_heads * HEAD_WIDTH,
            transcendentals=0,
        ),
        name="rope_pairs",
    )(*keys, *values, cosine, sine_part)
    gathered = [lax.all_gather(pair, "seq", axis=1, tiled=True) for pair in pairs]

    chunk_blocks = count_of_blocks // chunks
    mixed = [
        [
            attention_call(
                queries[chunk], cosine, sine_part, gathered[part], ids, counts,
                chunk * chunk_blocks, part, part_heads, groups,
            )
            for chunk in range(chunks)
        ]
        for part in range(parts)
    ]
    depth = part_heads * groups * HEAD_WIDTH

    def project(weight, chunk):
        total = None
        for part in range(parts):
            term = jnp.dot(
                mixed[part][chunk],
                weight[part * depth : (part + 1) * depth],
                preferred_element_type=jnp.float32,
            )
            total = term if total is None else total + term
        return total

    results = []
    if head_count == 2:
        other_weight = lax.dynamic_slice_in_dim(w_output, (1 - head_index) * width_own, width_own, 1)
        own_weight = lax.dynamic_slice_in_dim(w_output, head_index * width_own, width_own, 1)
        for chunk in range(chunks):
            arrived = lax.ppermute(project(other_weight, chunk).astype(jnp.bfloat16), "head", swap)
            local = own_tokens[chunk].astype(jnp.float32) + project(own_weight, chunk)
            results.append((local + arrived.astype(jnp.float32)).astype(jnp.bfloat16))
    else:
        for chunk in range(chunks):
            summed = lax.psum_scatter(
                project(w_output, chunk).astype(jnp.bfloat16), "head", scatter_dimension=1, tiled=True
            )
            results.append(
                (own_tokens[chunk].astype(jnp.float32) + summed.astype(jnp.float32)).astype(jnp.bfloat16)
            )
    return jnp.concatenate(results, axis=0)


def near_planes(blocks):
    return -(-(WINDOW_BLOCKS - 1) // (PLANE * blocks))


def exchange_kernel(
    planes, near, heads, groups, blocks,
    pick_ref, tok_hbm, gain_ref, cos_ref, sin_ref, wq_hbm, wk_hbm, wv_hbm,
    kv_hbm, q_ref,
    tok, normed, wq, wkv, own, stage,
    send, recv, far_send, far_recv, local_sem, weight_sem,
):
    seq, head = lax.axis_index("seq"), lax.axis_index("head")
    plane, me = seq // PLANE, lax.rem(seq, PLANE)
    across = lax.rem(me + PLANE // 2, PLANE)
    beside = me + 1 - 2 * lax.rem(me, 2)
    half_width = tok.shape[2]
    kv_width = heads * HEAD_WIDTH
    rows_of = lambda k: pl.ds(pl.multiple_of(k * BLOCK_TOKENS, BLOCK_TOKENS), BLOCK_TOKENS)
    base = plane * PLANE
    far_base = (near + 1) * PLANE * blocks

    def slot(d, member, k):
        return (d * PLANE + member) * blocks + k

    def remote(src, dst, kind, k, target, target_head):
        return pltpu.make_async_remote_copy(
            src_ref=src, dst_ref=dst, send_sem=send.at[kind, k], recv_sem=recv.at[kind, k],
            device_id=(target, target_head), device_id_type=MESH,
        )

    def token_copy(k):
        return remote(tok_hbm.at[rows_of(k), :], tok.at[head, rows_of(k), :], 0, k, seq, 1 - head)

    def up(d, k):
        src = own.at[k] if d == 1 else kv_hbm.at[slot(d - 1, me, k)]
        return remote(src, kv_hbm.at[slot(d, me, k)], d, k, seq + PLANE, head)

    def cross(d, k):
        at = slot(d, me, k)
        src = own.at[k] if d == 0 else kv_hbm.at[at]
        return remote(src, kv_hbm.at[at], near + 1 + d, k, base + across, head)

    def twin(d, crossed, k):
        at = slot(d, across if crossed else me, k)
        src = own.at[k] if d == 0 and not crossed else kv_hbm.at[at]
        return remote(src, kv_hbm.at[at], 2 * near + 2 + 2 * d + crossed, k, base + beside, head)

    def far_copy(d, j):
        index = (d - near - 1) * PLANE + j
        target = (plane + d) * PLANE + lax.rem(me + j, PLANE)
        return pltpu.make_async_remote_copy(
            src_ref=stage.at[index], dst_ref=kv_hbm.at[far_base + (d - near - 1) * PLANE + me],
            send_sem=far_send.at[index], recv_sem=far_recv.at[index],
            device_id=(target, head), device_id_type=MESH,
        )

    def keep(k):
        return pltpu.make_async_copy(own.at[k], kv_hbm.at[slot(0, me, k)], local_sem.at[k])

    half_copy = pltpu.make_async_copy(tok_hbm, tok.at[head], weight_sem.at[0])
    key_copy = pltpu.make_async_copy(wk_hbm, wkv.at[:, pl.ds(0, kv_width)], weight_sem.at[1])
    value_copy = pltpu.make_async_copy(wv_hbm, wkv.at[:, pl.ds(kv_width, kv_width)], weight_sem.at[2])
    query_copy = pltpu.make_async_copy(wq_hbm, wq, weight_sem.at[3])
    half_copy.start()
    key_copy.start()
    value_copy.start()
    query_copy.start()

    barrier = pltpu.get_barrier_semaphore()

    def greet(target, target_head):
        pl.semaphore_signal(barrier, inc=1, device_id=(target, target_head), device_id_type=MESH)

    greet(seq, 1 - head)
    greet(base + across, head)
    greet(base + beside, head)
    ahead = [1] + list(range(near + 1, planes))
    for d in ahead:
        members = [me] if d == 1 else [lax.rem(me + j, PLANE) for j in range(PLANE)]

        @pl.when(plane + d < planes)
        def _():
            for member in members:
                greet((plane + d) * PLANE + member, head)

        @pl.when(plane >= d)
        def _():
            for member in members:
                greet((plane - d) * PLANE + member, head)

    peers = 3
    for d in ahead:
        sides = (plane + d < planes).astype(jnp.int32) + (plane >= d).astype(jnp.int32)
        peers = peers + sides * (1 if d == 1 else PLANE)
    pl.semaphore_wait(barrier, peers)

    @pl.loop(0, blocks)
    def _(k):
        token_copy(k).start()

    half_copy.wait()
    key_copy.wait()
    value_copy.wait()
    tiles = heads * groups * HEAD_WIDTH // QUERY_TILE
    share = -(-tiles // (near + 1))

    @pl.loop(0, blocks + near + 1)
    def _(t):
        @pl.when(t < blocks)
        def _():
            token_copy(t).wait_recv()
            rows = rows_of(t)
            square = None
            for side in range(2):
                wide = tok[side, rows, :].astype(jnp.float32)
                part = jnp.sum(wide * wide, axis=1, keepdims=True)
                square = part if square is None else square + part
            scale = lax.rsqrt(square / MODEL_WIDTH + EPSILON)
            total = None
            for side in range(2):
                span = slice(side * half_width, (side + 1) * half_width)
                wide = tok[side, rows, :].astype(jnp.float32)
                narrow = (wide * scale * gain_ref[:, span]).astype(jnp.bfloat16)
                normed[side, rows, :] = narrow
                term = jnp.dot(narrow, wkv[span, :], preferred_element_type=jnp.float32)
                total = term if total is None else total + term
            cosine, sine_part = cos_ref[rows, :], sin_ref[rows, :]
            for h in range(heads):
                u = total[:, h * HEAD_WIDTH : (h + 1) * HEAD_WIDTH]
                own[t, h] = turned(u, cosine, sine_part).astype(jnp.bfloat16)
                v = total[:, kv_width + h * HEAD_WIDTH : kv_width + (h + 1) * HEAD_WIDTH]
                own[t, heads + h] = v.T.astype(jnp.bfloat16)

            @pl.when(plane + 1 < planes)
            def _():
                up(1, t).start()

            cross(0, t).start()
            twin(0, 0, t).start()
            keep(t).start()

        for d in range(1, near + 1):
            @pl.when((t >= d) & (t < blocks + d) & (plane >= d))
            def _():
                k = t - d
                up(d, k).wait_recv()
                if d < near:
                    @pl.when(plane + 1 < planes)
                    def _():
                        up(d + 1, k).start()
                cross(d, k).start()
                twin(d, 0, k).start()

        for d in range(near + 1):
            @pl.when((t >= d + 1) & (t < blocks + d + 1) & (plane >= d))
            def _():
                k = t - d - 1
                cross(d, k).wait_recv()
                twin(d, 1, k).start()

        for d in range(near + 1, planes):
            @pl.when((t == blocks - 1) & (plane + d < planes))
            def _():
                for j in range(PLANE):
                    target = (plane + d) * PLANE + lax.rem(me + j, PLANE)
                    stage[(d - near - 1) * PLANE + j] = own[pick_ref[target]]

            @pl.when((t == blocks) & (plane + d < planes))
            def _():
                for j in range(PLANE):
                    far_copy(d, j).start()

        @pl.when(t == blocks)
        def _():
            query_copy.wait()

        @pl.when(t >= blocks)
        def _():
            @pl.loop((t - blocks) * share, jnp.minimum((t - blocks + 1) * share, tiles))
            def _(tile):
                columns = pl.ds(pl.multiple_of(tile * QUERY_TILE, QUERY_TILE), QUERY_TILE)
                total = jnp.dot(
                    normed[0], wq[0:half_width, columns], preferred_element_type=jnp.float32
                ) + jnp.dot(normed[1], wq[half_width:, columns], preferred_element_type=jnp.float32)
                for at in range(QUERY_TILE // HEAD_WIDTH):
                    which = tile * (QUERY_TILE // HEAD_WIDTH) + at
                    group = lax.rem(which, groups)
                    place = pl.ds(pl.multiple_of(group * HEAD_WIDTH, HEAD_WIDTH), HEAD_WIDTH)
                    u = total[:, at * HEAD_WIDTH : (at + 1) * HEAD_WIDTH]
                    ready = turned(u, cos_ref[...], sin_ref[...]) * SCORE_SCALE
                    for b in range(blocks):
                        one = ready[b * BLOCK_TOKENS : (b + 1) * BLOCK_TOKENS]
                        q_ref[which // groups, b, :, place] = one.T.astype(jnp.bfloat16)

    for d in range(near + 1, planes):
        @pl.when(plane >= d)
        def _():
            for j in range(PLANE):
                far_copy(d, j).wait_recv()

        @pl.when(plane + d < planes)
        def _():
            for j in range(PLANE):
                far_copy(d, j).wait_send()

    @pl.loop(0, blocks)
    def _(k):
        token_copy(k).wait_send()
        keep(k).wait()
        for d in range(near + 1):
            @pl.when(plane >= d)
            def _():
                cross(d, k).wait_send()
                for crossed in range(2):
                    twin(d, crossed, k).wait()
                if d < near:
                    @pl.when(plane + 1 < planes)
                    def _():
                        up(d + 1, k).wait_send()


def exchange(tokens, norm_gain, w_query, w_key, w_value, cosine, sine_part, pick):
    rows, width = tokens.shape
    blocks = rows // BLOCK_TOKENS
    heads = w_key.shape[1] // HEAD_WIDTH
    groups = w_query.shape[1] // w_key.shape[1]
    planes = lax.axis_size("seq") // PLANE
    near = near_planes(blocks)
    far = max(planes - near - 1, 0)
    slots = (near + 1) * PLANE * blocks + far * PLANE
    piece = (2 * heads, BLOCK_TOKENS, HEAD_WIDTH)
    anywhere, vmem = pl.BlockSpec(memory_space=pl.ANY), pl.BlockSpec(memory_space=pltpu.VMEM)
    kinds = 4 * near + 4
    return pl.pallas_call(
        functools.partial(exchange_kernel, planes, near, heads, groups, blocks),
        out_shape=[
            jax.ShapeDtypeStruct((slots,) + piece, jnp.bfloat16),
            jax.ShapeDtypeStruct((heads, blocks, HEAD_WIDTH, groups * BLOCK_TOKENS), jnp.bfloat16),
        ],
        in_specs=[pl.BlockSpec(memory_space=pltpu.SMEM), anywhere, vmem, vmem, vmem] + [anywhere] * 3,
        out_specs=[anywhere, vmem],
        scratch_shapes=[
            pltpu.VMEM((2, rows, width), jnp.bfloat16),
            pltpu.VMEM((2, rows, width), jnp.bfloat16),
            pltpu.VMEM(w_query.shape, jnp.bfloat16),
            pltpu.VMEM((w_key.shape[0], 2 * w_key.shape[1]), jnp.bfloat16),
            pltpu.VMEM((blocks,) + piece, jnp.bfloat16),
            pltpu.VMEM((max(far, 1) * PLANE,) + piece, jnp.bfloat16),
            pltpu.SemaphoreType.DMA((kinds, blocks)),
            pltpu.SemaphoreType.DMA((kinds, blocks)),
            pltpu.SemaphoreType.DMA((max(far, 1) * PLANE,)),
            pltpu.SemaphoreType.DMA((max(far, 1) * PLANE,)),
            pltpu.SemaphoreType.DMA((blocks,)),
            pltpu.SemaphoreType.DMA((4,)),
        ],
        compiler_params=pltpu.CompilerParams(
            collective_id=0, has_side_effects=True, vmem_limit_bytes=EXCHANGE_VMEM
        ),
        cost_estimate=pl.CostEstimate(
            flops=2 * rows * w_query.shape[0] * (w_query.shape[1] + 2 * w_key.shape[1]),
            bytes_accessed=2 * (w_query.size + 2 * w_key.size), transcendentals=0,
        ),
        name="exchange",
    )(pick, tokens, norm_gain[None, :], cosine, sine_part, w_query, w_key, w_value)


def blocks_kernel(
    heads, groups, first, turn_blocks, slot_ref, count_ref, q_ref, kv_ref, o_ref, m_s, l_s, acc_s
):
    block = pl.program_id(0) + first
    listed = count_ref[block]
    last = slot_ref.shape[1] - 1
    height = groups * BLOCK_TOKENS

    own = slot_ref[block, last]
    key_at = lax.broadcasted_iota(jnp.int32, (BLOCK_TOKENS, height), 0)
    row_at = lax.broadcasted_iota(jnp.int32, (BLOCK_TOKENS, height), 1) % BLOCK_TOKENS
    causal = key_at <= row_at
    scores = [
        jnp.dot(kv_ref[own, h], q_ref[h, 0], preferred_element_type=jnp.float32) for h in range(heads)
    ]
    for h in range(heads):
        one = jnp.where(causal, scores[h], NEGATIVE)
        top = jnp.max(one, axis=0, keepdims=True)
        weights = jnp.exp2(one - top)
        m_s[h] = top
        l_s[h] = jnp.sum(weights, axis=0, keepdims=True)
        acc_s[h] = jnp.dot(
            kv_ref[own, heads + h], weights.astype(jnp.bfloat16), preferred_element_type=jnp.float32
        )

    def turn(index, masked):
        at = index * turn_blocks
        slots = [slot_ref[block, at + j] for j in range(turn_blocks)]

        def score(h):
            keys = jnp.concatenate([kv_ref[one, h] for one in slots], axis=0)
            return jnp.dot(keys, q_ref[h, 0], preferred_element_type=jnp.float32)

        ready = score(0)
        for h in range(heads):
            one = ready
            if h + 1 < heads:
                ready = score(h + 1)
            if masked:
                key = lax.broadcasted_iota(jnp.int32, one.shape, 0)
                one = jnp.where(key < (listed - at) * BLOCK_TOKENS, one, NEGATIVE)
            top_prev = m_s[h]
            top = jnp.maximum(top_prev, jnp.max(one, axis=0, keepdims=True))
            factor = jnp.exp2(top_prev - top)
            weights = jnp.exp2(one - top)
            m_s[h] = top
            l_s[h] = l_s[h] * factor + jnp.sum(weights, axis=0, keepdims=True)
            values = jnp.concatenate([kv_ref[one_slot, heads + h] for one_slot in slots], axis=1)
            acc_s[h] = acc_s[h] * factor + jnp.dot(
                values, weights.astype(jnp.bfloat16), preferred_element_type=jnp.float32
            )

    whole = listed // turn_blocks

    @pl.loop(0, whole)
    def _(index):
        turn(index, False)

    @pl.when(listed > whole * turn_blocks)
    def _():
        turn(whole, True)

    for h in range(heads):
        done = acc_s[h] / l_s[h]
        for group in range(groups):
            span = slice(group * BLOCK_TOKENS, (group + 1) * BLOCK_TOKENS)
            column = (h * groups + group) * HEAD_WIDTH
            o_ref[:, column : column + HEAD_WIDTH] = done[:, span].T.astype(jnp.bfloat16)


def blocks_call(query, gathered, slots, counts, first, count):
    heads, _, width, height = query.shape
    groups = height // BLOCK_TOKENS
    whole = gathered.shape
    grid_spec = pltpu.PrefetchScalarGridSpec(
        num_scalar_prefetch=2,
        grid=(count,),
        in_specs=[
            pl.BlockSpec((heads, 1, width, height), lambda b, *_: (0, first + b, 0, 0)),
            pl.BlockSpec(whole, lambda b, *_: (0, 0, 0, 0), pipeline_mode=pl.Buffered(1)),
        ],
        out_specs=pl.BlockSpec((BLOCK_TOKENS, heads * height), lambda b, *_: (b, 0)),
        scratch_shapes=[
            pltpu.VMEM((heads, 1, height), jnp.float32),
            pltpu.VMEM((heads, 1, height), jnp.float32),
            pltpu.VMEM((heads, width, height), jnp.float32),
        ],
    )
    pairs = heads * height * count * BLOCK_TOKENS * WINDOW_BLOCKS // 2
    return pl.pallas_call(
        functools.partial(blocks_kernel, heads, groups, first, TURN),
        grid_spec=grid_spec,
        out_shape=jax.ShapeDtypeStruct((count * BLOCK_TOKENS, heads * height), jnp.bfloat16),
        compiler_params=pltpu.CompilerParams(
            dimension_semantics=("arbitrary",), vmem_limit_bytes=VMEM_BYTES
        ),
        cost_estimate=pl.CostEstimate(
            flops=pairs * HEAD_WIDTH * 4, bytes_accessed=gathered.size * 2, transcendentals=pairs
        ),
        name="attention",
    )(slots, counts, query, gathered)


def slot_lists(ids, seq_index, blocks, near):
    owner = ids // blocks
    distance = seq_index // PLANE - owner // PLANE
    member = owner % PLANE
    close = (distance * PLANE + member) * blocks + ids % blocks
    distant = (near + 1) * PLANE * blocks + (distance - near - 1) * PLANE + member
    return jnp.where(distance <= near, close, distant)


def shards(tokens, norm_gain, w_query, w_key, w_value, w_output, widths, dilation):
    row_count, width_own = tokens.shape
    blocks = row_count // BLOCK_TOKENS
    seq_index, head_index = lax.axis_index("seq"), lax.axis_index("head")
    first_block = seq_index * blocks
    swap = [(0, 1), (1, 0)]
    near = near_planes(blocks)

    half = HEAD_WIDTH // 2
    lane = jnp.arange(HEAD_WIDTH, dtype=jnp.int32)
    frequency = ROPE_BASE ** (-(lane % half).astype(jnp.float32) * 2.0 / HEAD_WIDTH)
    positions = first_block * BLOCK_TOKENS + jnp.arange(row_count, dtype=jnp.int32)
    angles = positions.astype(jnp.float32)[:, None] * frequency[None, :]
    cosine = jnp.cos(angles)
    sine_part = jnp.sin(angles) * jnp.where(lane < half, -1.0, 1.0)[None, :]

    mine = dilation // blocks == seq_index
    pick = jnp.max(jnp.where(mine, dilation % blocks, 0).reshape(lax.axis_size("seq"), -1), axis=1)
    gathered, query = exchange(
        tokens, norm_gain, w_query, w_key, w_value, cosine, sine_part, pick
    )
    ids, counts = block_lists(first_block, blocks, widths, dilation)
    place = jnp.arange(ids.shape[1], dtype=jnp.int32)
    ids = jnp.where(place[None, :] < counts[:, None], ids, ids[:, -1:])
    slots = slot_lists(ids, seq_index, blocks, near)

    other_weight = lax.dynamic_slice_in_dim(w_output, (1 - head_index) * width_own, width_own, 1)
    own_weight = lax.dynamic_slice_in_dim(w_output, head_index * width_own, width_own, 1)
    chunks = 2 if blocks % 2 == 0 else 1
    count, rows = blocks // chunks, row_count // chunks
    results = []
    for chunk in range(chunks):
        mixed = blocks_call(query, gathered, slots, counts, chunk * count, count)
        other = jnp.dot(mixed, other_weight, preferred_element_type=jnp.float32)
        arrived = lax.ppermute(other.astype(jnp.bfloat16), "head", swap)
        local = tokens[chunk * rows : (chunk + 1) * rows].astype(jnp.float32) + jnp.dot(
            mixed, own_weight, preferred_element_type=jnp.float32
        )
        results.append((local + arrived.astype(jnp.float32)).astype(jnp.bfloat16))
    return jnp.concatenate(results, axis=0)


def solution(mesh):
    paired = mesh.shape["head"] == 2 and mesh.shape["seq"] % PLANE == 0
    body = shards if paired else general_shards
    in_specs = (
        P("seq", "head"),
        P(),
        P(None, "head"),
        P(None, "head"),
        P(None, "head"),
        P("head", None),
        P("seq"),
        P(),
    )
    out_specs = P("seq", "head")
    return jax.shard_map(body, mesh=mesh, in_specs=in_specs, out_specs=out_specs, check_vma=False)
```
